32 devices in a mesh: group: 2 (over y), expert: 4 (over z), tensor: 4 (over x, core).
Axes of the slice: x: 2, y: 2, z: 4, core: 2. Of those that a mesh axis runs over, the one named last changes fastest.
Arguments:
- tokens: bfloat16 [2048, 4096], P(('group', 'expert', 'tensor')), parts along dimension 0, may hold values from -6 to 6
- cotangent: bfloat16 [2048, 4096], P(('group', 'expert', 'tensor')), parts along dimension 0, may hold values from -6 to 6
- expert_ids: int32 [2048, 2], P(('group', 'expert', 'tensor')), parts along dimension 0, may hold values from 0 to 3, all different within a row
- gate_wts: float32 [2048, 2], P(('group', 'expert', 'tensor')), parts along dimension 0, may hold values from 0.2 to 1
- w_gate: bfloat16 [4, 4096, 256], P('expert', 'tensor'), may hold values from -0.09375 to 0.09375
- w_up: bfloat16 [4, 4096, 256], P('expert', 'tensor'), may hold values from -0.09375 to 0.09375
- w_down: bfloat16 [4, 256, 4096], P('expert', 'tensor'), may hold values from -0.375 to 0.375
Outputs:
- input_grad: bfloat16 [2048, 4096], P(('group', 'expert', 'tensor')), parts along dimension 0
- grad_gate: bfloat16 [8, 4096, 256], P(('group', 'expert'), 'tensor'), parts along dimension 0
- grad_up: bfloat16 [8, 4096, 256], P(('group', 'expert'), 'tensor'), parts along dimension 0
- grad_down: bfloat16 [8, 256, 4096], P(('group', 'expert'), 'tensor'), parts along dimension 0
The draws below stay inside these ranges and needn't reach their ends.
There are 2 independent parts, one for each index of `group`. The reference program is written for one: setup_inputs(seed, part) draws one part's arguments, and reference() takes and returns one part's arrays. A program takes and returns all parts, laid end to end along the dimension named above; an argument that names none is the same for every part. Nothing has to cross between parts.
Inputs may be any that keep to these rules, and one draw needn't show every extreme that they name: `expert_ids`: the two ids of a token differ.
All inputs are finite; a program needn't handle non-finite values.
Results may differ from the reference program's by a relative error of at most 0.009.
Values may be sent and summed in bfloat16 or wider, within the bound.
A program may use at most 64 MiB of HBM per device.

```python
import jax
import jax.numpy as jnp
from jax import lax

D = 4096
FF = 256
TOK_DEV = 64
EXPERTS = 4
CAP = 32
TOKENS = 1024
N_EXPERT = 4
N_TENSOR = 4


def block_levels(key, shape, pieces, least, top_value):
    factor_of, own = 1.0, jax.random.fold_in(key, 6)
    for position, blocks in pieces:
        steps = jnp.exp(jax.random.uniform(jax.random.fold_in(own, position), (blocks,), jnp.float32, least / len(pieces), top_value / len(pieces)))
        factor_of = factor_of * jnp.repeat(steps, shape[position] // blocks).reshape([-1 if axis == position else 1 for axis in range(len(shape))])
    return factor_of


def different_ones(key, rows, amount, top, lift):
    ranking = jax.random.permutation(jax.random.fold_in(key, 1), amount)
    pull = ranking
    for power in range(3):
        pull = pull * pull // amount
    pull = pull * lift // amount
    chance = jax.random.randint(jax.random.fold_in(key, 2), (rows, amount), 0, 4096) + pull
    holders = jax.random.permutation(jax.random.fold_in(key, 3), rows)[jnp.arange(amount) % rows]
    chance = jnp.where(jnp.arange(rows)[:, None] == holders[None, :], 1 << 14, chance)
    priority = chance * amount + jnp.arange(amount)
    return lax.top_k(priority.astype(jnp.int32), top)[1].astype(jnp.int32)


def gaussian(stream_key, extent, spread, limit, pieces=(), kind=jnp.bfloat16):
    level = block_levels(stream_key, extent, pieces, -0.22, 0.18) if pieces else 1.0
    drawn = jax.random.normal(stream_key, extent, jnp.float32) * spread * level
    return jnp.minimum(jnp.maximum(drawn, -limit), limit).astype(kind)


def setup_inputs(seed: int = 0, part: int = 0) -> dict:
    seeds = jax.random.split(jax.random.key(seed), 8)
    part_splits = jax.random.split(jax.random.fold_in(seeds[7], part), 8)
    return {
        "tokens": gaussian(part_splits[0], (TOKENS, D), 1.0, 6.0, ((0, 16),)),
        "cotangent": gaussian(part_splits[1], (TOKENS, D), 1.0, 6.0, ((0, 16),)),
        "expert_ids": different_ones(part_splits[2], TOKENS, EXPERTS, 2, 4096),
        "gate_wts": jnp.clip(0.2 + 0.8 * jax.random.uniform(part_splits[3], (TOKENS, 2), jnp.float32) ** block_levels(part_splits[3], (TOKENS, 2), ((0, 16),), -0.2, 0.2), 0.2, 1.0),
        "w_gate": gaussian(seeds[4], (EXPERTS, D, FF), D ** -0.5, 0.09375, ((0, 4), (1, 4))),
        "w_up": gaussian(seeds[5], (EXPERTS, D, FF), D ** -0.5, 0.09375, ((0, 4), (1, 4))),
        "w_down": gaussian(seeds[6], (EXPERTS, FF, D), FF ** -0.5, 0.375, ((0, 4), (1, 4))),
    }


def reference(tokens, cotangent, expert_ids, gate_wts, w_gate, w_up, w_down):
    sources = N_EXPERT * N_TENSOR
    model_width = tokens.shape[1]
    slots_all = EXPERTS * CAP
    flat_ids = expert_ids.reshape(sources, 2 * TOK_DEV)
    onehot = (flat_ids[:, :, None] == jnp.arange(EXPERTS, dtype=jnp.int32)[None, None, :]).astype(jnp.int32)
    positions = jnp.sum(onehot * (jnp.cumsum(onehot, axis=1) - 1), axis=2)
    retained = positions < CAP
    target = jnp.where(retained, flat_ids * CAP + positions, slots_all)

    def invert(row_target):
        return jnp.full((slots_all,), -1, jnp.int32).at[row_target].set(
            jnp.arange(2 * TOK_DEV, dtype=jnp.int32), mode="drop")

    anchor = jax.vmap(invert)(target)
    gate_flat = gate_wts.reshape(sources, 2 * TOK_DEV)
    block_base = (jnp.arange(sources, dtype=jnp.int32) * TOK_DEV)[:, None]
    zero_half = jnp.zeros((), jnp.bfloat16)

    def partial_sum(left, right):
        left_transposed = left.reshape(N_EXPERT, N_TENSOR, CAP, -1).transpose(1, 0, 2, 3)
        left_transposed = left_transposed.reshape(N_TENSOR, N_EXPERT * CAP, -1).astype(jnp.float32)
        right_transposed = right.reshape(N_EXPERT, N_TENSOR, CAP, -1).transpose(1, 0, 2, 3)
        right_transposed = right_transposed.reshape(N_TENSOR, N_EXPERT * CAP, -1).astype(jnp.float32)
        summands = jnp.einsum("aye,aym->aem", left_transposed, right_transposed).astype(jnp.bfloat16)
        summands = lax.optimization_barrier(summands)
        return jnp.sum(summands.astype(jnp.float32), axis=0).astype(jnp.bfloat16)

    def one_expert(expert):
        chosen = lax.dynamic_slice_in_dim(anchor, expert * CAP, CAP, 1)
        populated_rows = (chosen >= 0).reshape(-1)
        picked = jnp.maximum(chosen, 0)
        tok_index = (block_base + picked // 2).reshape(-1)
        rows_in = jnp.where(populated_rows[:, None], tokens[tok_index], zero_half)
        gate_scale = jnp.take_along_axis(gate_flat, picked, axis=1).reshape(-1)
        scaled = (gate_scale[:, None] * cotangent[tok_index].astype(jnp.float32)).astype(jnp.bfloat16)
        cot_in = jnp.where(populated_rows[:, None], scaled, zero_half)
        gate_matrix = w_gate[expert]
        up_mat = w_up[expert]
        down_mat = w_down[expert]
        pre_gate = jnp.dot(rows_in, gate_matrix, preferred_element_type=jnp.float32)
        pre_up = jnp.dot(rows_in, up_mat, preferred_element_type=jnp.float32)
        sigmoid_gate = jax.nn.sigmoid(pre_gate)
        activated = pre_gate * sigmoid_gate
        hidden = (activated * pre_up).astype(jnp.bfloat16)
        grad_hidden = jnp.dot(cot_in, down_mat.T, preferred_element_type=jnp.float32)
        grad_gate_pre = (grad_hidden * pre_up * sigmoid_gate * (1.0 + pre_gate * (1.0 - sigmoid_gate))).astype(jnp.bfloat16)
        grad_up_pre = (grad_hidden * activated).astype(jnp.bfloat16)
        input_rows = (jnp.dot(grad_gate_pre, gate_matrix.T, preferred_element_type=jnp.float32)
                      + jnp.dot(grad_up_pre, up_mat.T, preferred_element_type=jnp.float32)).astype(jnp.bfloat16)
        return (partial_sum(rows_in, grad_gate_pre), partial_sum(rows_in, grad_up_pre),
                partial_sum(hidden, cot_in), input_rows.reshape(sources, CAP, model_width))

    grad_gate, grad_up, grad_down, input_all = lax.map(one_expert, jnp.arange(EXPERTS, dtype=jnp.int32))
    slot_clip = jnp.minimum(positions, CAP - 1).astype(jnp.int32)
    source_index = jnp.broadcast_to(jnp.arange(sources, dtype=jnp.int32)[:, None], flat_ids.shape)
    gathered = input_all[flat_ids, source_index, slot_clip].astype(jnp.float32)
    gathered = jnp.where(retained[:, :, None], gathered, jnp.zeros((), jnp.float32))
    input_grad = jnp.sum(gathered.reshape(sources, TOK_DEV, 2, model_width), axis=2)
    input_grad = input_grad.reshape(TOKENS, model_width).astype(jnp.bfloat16)
    return (input_grad, grad_gate, grad_up, grad_down)
```

```python
import jax
import jax.numpy as jnp
from jax import lax
from jax.experimental import pallas as pl
from jax.experimental.pallas import tpu as pltpu
from jax.sharding import PartitionSpec as P

MESH = pl.DeviceIdType.MESH
SEND_ORDER = (2, 3, 1, 0)
WORK_ORDER = (2, 1, 0, 3)


def contract_last(left, right):
    return lax.dot_general(
        left, right, (((1,), (1,)), ((), ())), preferred_element_type=jnp.float32
    )


def contract_first(left, right):
    return lax.dot_general(
        left, right, (((0,), (0,)), ((), ())), preferred_element_type=jnp.float32
    )


def dot(left, right):
    return jnp.dot(left, right, preferred_element_type=jnp.float32)


def flip(index, mask):
    out = index
    for bit in (1, 2):
        if mask & bit:
            out = out + bit - 2 * bit * ((index // bit) % 2)
    return out


def kernel(
    tok, cot, ids, gat, wg, wu, wd,
    ig, gg, gu, gd,
    srow, scot, rrow, rcot, wdf, part, par, pbs, pbr, act, rets, retr, gds, gdr,
    d_ss, d_rs, w_ss, w_rs, a_ss, a_rs, b_ss, b_rs, c_ss, c_rs, r_ss, r_rs, g_ss, g_rs, l_s,
):
    n_exp, n_ten = 4, 4
    toks, width = tok.shape
    cols = width // n_ten
    cap = srow.shape[1]
    half = n_ten * cap // 2
    ff_t = wd.shape[1]
    g = lax.axis_index("group")
    e = lax.axis_index("expert")
    t = lax.axis_index("tensor")
    ex = [flip(e, r) for r in range(n_exp)]
    tx = [flip(t, q) for q in range(n_ten)]

    def dcol(q):
        return pl.ds(pl.multiple_of(tx[q] * cols, cols), cols)

    def drow(q):
        return pl.ds(pl.multiple_of(tx[q] * cap, cap), cap)

    def dff(q):
        return pl.ds(pl.multiple_of(tx[q] * ff_t, ff_t), ff_t)

    sends = []

    def remote(src, dst, ss, rs, r, q):
        c = pltpu.make_async_remote_copy(
            src_ref=src, dst_ref=dst, send_sem=ss, recv_sem=rs,
            device_id=(g, ex[r], tx[q]), device_id_type=MESH,
        )
        c.start()
        sends.append(c)
        return c

    def move(src, dst, sem):
        c = pltpu.make_async_copy(src, dst, sem)
        c.start()
        return c

    barrier = pltpu.get_barrier_semaphore()
    for r in range(n_exp):
        for q in range(n_ten):
            if r or q:
                pl.semaphore_signal(
                    barrier, inc=1, device_id=(g, ex[r], tx[q]), device_id_type=MESH
                )

    id0, id1 = ids[0:1, :], ids[1:2, :]
    lab = lax.broadcasted_iota(jnp.int32, (8, toks), 0)
    oh0 = (jnp.broadcast_to(id0, (8, toks)) == lab).astype(jnp.float32)
    oh1 = (jnp.broadcast_to(id1, (8, toks)) == lab).astype(jnp.float32)
    before = (
        lax.broadcasted_iota(jnp.int32, (toks, toks), 0)
        < lax.broadcasted_iota(jnp.int32, (toks, toks), 1)
    ).astype(jnp.bfloat16)
    count = dot((oh0 + oh1).astype(jnp.bfloat16), before)
    p0 = jnp.sum(oh0 * count, axis=0, keepdims=True)
    p1 = jnp.sum(oh1 * (count + oh0), axis=0, keepdims=True)
    none = -1.0
    s0 = jnp.where(p0 < cap, id0.astype(jnp.float32) * cap + p0, none)
    s1 = jnp.where(p1 < cap, id1.astype(jnp.float32) * cap + p1, none)
    gate0, gate1 = gat[0:1, :], gat[1:2, :]

    def place(r):
        slot = (ex[r] * cap + lax.broadcasted_iota(jnp.int32, (cap, toks), 0)).astype(jnp.float32)
        return slot == jnp.broadcast_to(s0, (cap, toks)), slot == jnp.broadcast_to(s1, (cap, toks))

    disp, wcp, locs = {}, {}, {}
    picks = {}
    first = True
    for r in SEND_ORDER:
        m0, m1 = place(r)
        pick = (m0 | m1).astype(jnp.bfloat16)
        picks[r] = pick
        scale = jnp.sum(
            jnp.where(m0, jnp.broadcast_to(gate0, m0.shape), 0.0)
            + jnp.where(m1, jnp.broadcast_to(gate1, m1.shape), 0.0),
            axis=1, keepdims=True,
        )
        srow[r] = dot(pick, tok[...]).astype(jnp.bfloat16)
        scot[r] = (scale * dot(pick, cot[...])).astype(jnp.bfloat16)
        if first:
            pl.semaphore_wait(barrier, n_exp * n_ten - 1)
            first = False
        for q in (3, 2, 1, 0):
            for k, (sb, rb) in enumerate(((srow, rrow), (scot, rcot))):
                src = sb.at[r, :, dcol(q)]
                dst = rb.at[r, drow(0), :]
                if r or q:
                    disp[k, r, q] = remote(src, dst, d_ss.at[k, r, q], d_rs.at[k, r, q], r, q)
                else:
                    locs["d", k] = move(src, dst, l_s.at[k])
        if r == SEND_ORDER[0]:
            for q in (3, 2, 1, 0):
                src = wd.at[0, :, dcol(q)]
                dst = wdf.at[dff(0), :]
                if q:
                    wcp[q] = remote(src, dst, w_ss.at[q], w_rs.at[q], 0, q)
                else:
                    locs["w"] = move(src, dst, l_s.at[2])

    odd = t % 2
    mine = pl.ds(pl.multiple_of(odd * half, half), half)
    other = pl.ds(pl.multiple_of((1 - odd) * half, half), half)

    rcp = {}
    for pos, r in enumerate(WORK_ORDER):
        for q in range(n_ten):
            for k in range(2):
                if r or q:
                    disp[k, r, q].wait_recv()
                else:
                    locs["d", k].wait()
        if pos == 0:
            locs["w"].wait()
            for q in range(1, n_ten):
                wcp[q].wait_recv()
        x = rrow[r]
        part[r, 0] = dot(x, wg[0])
        part[r, 1] = dot(x, wu[0])
        part[r, 2] = contract_last(rcot[r], wdf[...])
        a = remote(part.at[r, :, other, :], par.at[r], a_ss.at[r], a_rs.at[r], 0, 1)
        a.wait_recv()
        total = part[r, :, mine, :] + par[r]
        pbs[r] = total.astype(jnp.bfloat16)
        b = remote(pbs.at[r], pbr.at[r], b_ss.at[r], b_rs.at[r], 0, 2)
        b.wait_recv()
        total = total + pbr[r].astype(jnp.float32)
        pre_gate, pre_up, grad_hidden = total[0], total[1], total[2]
        sig = jax.nn.sigmoid(pre_gate)
        silu = pre_gate * sig
        act[r, 0, mine, :] = (silu * pre_up).astype(jnp.bfloat16)
        act[r, 1, mine, :] = (
            grad_hidden * pre_up * sig * (1.0 + pre_gate * (1.0 - sig))
        ).astype(jnp.bfloat16)
        act[r, 2, mine, :] = (grad_hidden * silu).astype(jnp.bfloat16)
        c = remote(act.at[r, :, mine, :], act.at[r, :, mine, :], c_ss.at[r], c_rs.at[r], 0, 1)
        c.wait_recv()
        rets[r] = (contract_last(act[r, 1], wg[0]) + contract_last(act[r, 2], wu[0])).astype(
            jnp.bfloat16
        )
        for q in (3, 2, 1, 0):
            src = rets.at[r, drow(q), :]
            dst = retr.at[r, :, dcol(0)]
            if r or q:
                rcp[r, q] = remote(src, dst, r_ss.at[r, q], r_rs.at[r, q], r, q)
            else:
                locs["r"] = move(src, dst, l_s.at[3])

    slots = n_exp * n_ten * cap
    wide = act.shape[3]
    cot_all = rcot[...].reshape(slots, cols)
    hid = act[:, 0].reshape(slots, wide)
    gds[...] = contract_first(hid, cot_all).astype(jnp.bfloat16)
    gcp = {}
    for q in (3, 2, 1, 0):
        src = gds.at[dff(q), :]
        dst = gdr.at[:, dcol(0)]
        if q:
            gcp[q] = remote(src, dst, g_ss.at[q], g_rs.at[q], 0, q)
        else:
            locs["g"] = move(src, dst, l_s.at[4])
    rows_all = rrow[...].reshape(slots, cols)
    gg[0] = contract_first(rows_all, act[:, 1].reshape(slots, wide)).astype(jnp.bfloat16)
    gu[0] = contract_first(rows_all, act[:, 2].reshape(slots, wide)).astype(jnp.bfloat16)

    locs["g"].wait()
    for q in range(1, n_ten):
        gcp[q].wait_recv()
    gd[0] = gdr[...]
    locs["r"].wait()
    for r in range(n_exp):
        for q in range(n_ten):
            if r or q:
                rcp[r, q].wait_recv()
    pick = jnp.concatenate([picks[r] for r in range(n_exp)], axis=0)
    ig[...] = contract_first(pick, retr[...].reshape(n_exp * cap, width)).astype(jnp.bfloat16)
    for c in sends:
        c.wait_send()


def fused(tokens, cotangent, expert_ids, gate_wts, w_gate, w_up, w_down):
    toks, width = tokens.shape
    n = 4
    cap = 2 * toks // n
    cols = w_gate.shape[1]
    wide = w_gate.shape[2]
    half = n * cap // 2
    bf, f32 = jnp.bfloat16, jnp.float32
    dma = pltpu.SemaphoreType.DMA
    vmem = pl.BlockSpec(memory_space=pltpu.VMEM)
    return pl.pallas_call(
        kernel,
        out_shape=(
            jax.ShapeDtypeStruct(tokens.shape, bf),
            jax.ShapeDtypeStruct(w_gate.shape, bf),
            jax.ShapeDtypeStruct(w_up.shape, bf),
            jax.ShapeDtypeStruct(w_down.shape, bf),
        ),
        in_specs=[vmem] * 7,
        out_specs=(vmem,) * 4,
        scratch_shapes=[
            pltpu.VMEM((n, cap, width), bf),
            pltpu.VMEM((n, cap, width), bf),
            pltpu.VMEM((n, n * cap, cols), bf),
            pltpu.VMEM((n, n * cap, cols), bf),
            pltpu.VMEM((wide, cols), bf),
            pltpu.VMEM((n, 3, n * cap, wide), f32),
            pltpu.VMEM((n, 3, half, wide), f32),
            pltpu.VMEM((n, 3, half, wide), bf),
            pltpu.VMEM((n, 3, half, wide), bf),
            pltpu.VMEM((n, 3, n * cap, wide), bf),
            pltpu.VMEM((n, n * cap, cols), bf),
            pltpu.VMEM((n, cap, width), bf),
            pltpu.VMEM((wide, cols), bf),
            pltpu.VMEM(w_down.shape[1:], bf),
            dma((2, n, n)), dma((2, n, n)),
            dma((n,)), dma((n,)),
            dma((n,)), dma((n,)),
            dma((n,)), dma((n,)),
            dma((n,)), dma((n,)),
            dma((n, n)), dma((n, n)),
            dma((n,)), dma((n,)),
            dma((5,)),
        ],
        compiler_params=pltpu.CompilerParams(
            collective_id=0, has_side_effects=True, vmem_limit_bytes=48 * 1024 * 1024
        ),
        name="expert_backward",
    )(tokens, cotangent, expert_ids.T, gate_wts.T, w_gate, w_up, w_down)


def plain(tokens, cotangent, expert_ids, gate_wts, w_gate, w_up, w_down):
    tok_rows, model_width = tokens.shape
    experts = lax.axis_size("expert")
    capacity = 2 * tok_rows // experts
    slots_all = experts * capacity
    zero_half = jnp.zeros((), jnp.bfloat16)
    flat_ids = expert_ids.reshape(-1)
    onehot = (flat_ids[:, None] == jnp.arange(experts, dtype=jnp.int32)[None, :]).astype(jnp.int32)
    positions = jnp.sum(onehot * (jnp.cumsum(onehot, axis=0) - 1), axis=1)
    retained = positions < capacity
    target = jnp.where(retained, flat_ids * capacity + positions, slots_all)
    anchor = (
        jnp.full((slots_all,), -1, jnp.int32)
        .at[target]
        .set(jnp.arange(2 * tok_rows, dtype=jnp.int32), mode="drop")
    )
    populated_rows = anchor >= 0
    picked = jnp.maximum(anchor, 0)
    tok_index = picked // 2
    send_rows = jnp.where(populated_rows[:, None], tokens[tok_index], zero_half)
    gate_scale = gate_wts.reshape(-1)[picked]
    scaled = (gate_scale[:, None] * cotangent[tok_index].astype(jnp.float32)).astype(jnp.bfloat16)
    send_cot = jnp.where(populated_rows[:, None], scaled, zero_half)
    recv_rows, recv_cot = (
        lax.all_to_all(
            send_rows.reshape(experts, capacity, model_width),
            "expert",
            split_axis=0,
            concat_axis=0,
            tiled=True,
        ),
        lax.all_to_all(
            send_cot.reshape(experts, capacity, model_width),
            "expert",
            split_axis=0,
            concat_axis=0,
            tiled=True,
        ),
    )
    rows_in = recv_rows.reshape(slots_all, model_width)
    cot_in = recv_cot.reshape(slots_all, model_width)
    gate_shard = w_gate[0]
    up_shard = w_up[0]
    down_shard = w_down[0]
    hidden_width = gate_shard.shape[1]
    full_gate, full_up, complete_down_weight = (
        lax.all_gather(gate_shard, "tensor", axis=0, tiled=True),
        lax.all_gather(up_shard, "tensor", axis=0, tiled=True),
        lax.all_gather(down_shard, "tensor", axis=0, tiled=True),
    )
    pre_gate = jnp.dot(rows_in, full_gate, preferred_element_type=jnp.float32)
    pre_up = jnp.dot(rows_in, full_up, preferred_element_type=jnp.float32)
    grad_hidden = contract_last(cot_in, complete_down_weight)
    sigmoid_gate = jax.nn.sigmoid(pre_gate)
    activated = pre_gate * sigmoid_gate
    hidden = (activated * pre_up).astype(jnp.bfloat16)
    grad_gate_pre = (
        grad_hidden * pre_up * sigmoid_gate * (1.0 + pre_gate * (1.0 - sigmoid_gate))
    ).astype(jnp.bfloat16)
    grad_up_pre = (grad_hidden * activated).astype(jnp.bfloat16)
    joint_grad = jnp.concatenate([grad_gate_pre, grad_up_pre], axis=1)
    columns = rows_in
    summed = lax.psum_scatter(
        contract_first(columns, joint_grad).astype(jnp.bfloat16),
        "tensor",
        scatter_dimension=0,
        tiled=True,
    ).astype(jnp.float32)
    columns = hidden
    summed_down = lax.psum_scatter(
        contract_first(columns, cot_in).astype(jnp.bfloat16),
        "tensor",
        scatter_dimension=0,
        tiled=True,
    )
    rows_out = (
        contract_last(grad_gate_pre, full_gate) + contract_last(grad_up_pre, full_up)
    ).astype(jnp.bfloat16)
    returned = lax.all_to_all(
        rows_out.reshape(experts, capacity, model_width),
        "expert",
        split_axis=0,
        concat_axis=0,
        tiled=True,
    )
    returned = returned.reshape(slots_all, model_width)
    gathered = returned[jnp.minimum(target, slots_all - 1)].astype(jnp.float32)
    gathered = jnp.where(retained[:, None], gathered, jnp.zeros((), jnp.float32))
    input_grad = jnp.sum(gathered.reshape(tok_rows, 2, model_width), axis=1).astype(jnp.bfloat16)
    return (
        input_grad,
        summed[:, :hidden_width].astype(jnp.bfloat16)[None],
        summed[:, hidden_width:].astype(jnp.bfloat16)[None],
        summed_down[None],
    )


def solution(mesh):
    n_exp, n_ten = mesh.shape["expert"], mesh.shape["tensor"]

    def local(tokens, cotangent, expert_ids, gate_wts, w_gate, w_up, w_down):
        args = (tokens, cotangent, expert_ids, gate_wts, w_gate, w_up, w_down)
        capacity = 2 * tokens.shape[0] // n_exp
        small = n_exp == 4 and n_ten == 4 and capacity % 16 == 0
        return fused(*args) if small else plain(*args)

    return jax.shard_map(
        local,
        mesh=mesh,
        in_specs=(
            P(("group", "expert", "tensor"), None),
            P(("group", "expert", "tensor"), None),
            P(("group", "expert", "tensor"), None),
            P(("group", "expert", "tensor"), None),
            P("expert", "tensor", None),
            P("expert", "tensor", None),
            P("expert", "tensor", None),
        ),
        out_specs=(
            P(("group", "expert", "tensor"), None),
            P(("group", "expert"), "tensor", None),
            P(("group", "expert"), "tensor", None),
            P(("group", "expert"), "tensor", None),
        ),
        check_vma=False,
    )
```

```python
import jax
import jax.numpy as jnp
from jax import lax
from jax.experimental import pallas as pl
from jax.experimental.pallas import tpu as pltpu
from jax.sharding import PartitionSpec as P

MESH = pl.DeviceIdType.MESH


def contract_last(left, right):
    return lax.dot_general(
        left, right, (((1,), (1,)), ((), ())), preferred_element_type=jnp.float32
    )


def contract_first(left, right):
    return lax.dot_general(
        left, right, (((0,), (0,)), ((), ())), preferred_element_type=jnp.float32
    )


def dot(left, right):
    return jnp.dot(left, right, preferred_element_type=jnp.float32)


def flip(index, mask):
    out = index
    for bit in (1, 2):
        if mask & bit:
            out = out + bit - 2 * bit * ((index // bit) % 2)
    return out


def kernel(
    h_tok, h_cot, ids, gat, h_wg, h_wu, h_wd,
    ig, gg, gu, gd,
    tok, cot, wg, wu, srow, scot, rrow, rcot, wdf, part, par, pbs, pbr, act, rets, retr, gds, gdr,
    d_ss, d_rs, w_ss, w_rs, a_ss, a_rs, b_ss, b_rs, c_ss, c_rs, r_ss, r_rs, g_ss, g_rs, l_s,
):
    n_exp, n_ten = 4, 4
    toks, width = tok.shape
    cols = width // n_ten
    cap = srow.shape[1]
    half = n_ten * cap // 2
    ff_t = h_wd.shape[1]
    g = lax.axis_index("group")
    e = lax.axis_index("expert")
    t = lax.axis_index("tensor")
    ex = [flip(e, r) for r in range(n_exp)]
    tx = [flip(t, q) for q in range(n_ten)]

    def dcol(q):
        return pl.ds(pl.multiple_of(tx[q] * cols, cols), cols)

    def drow(q):
        return pl.ds(pl.multiple_of(tx[q] * cap, cap), cap)

    def dff(q):
        return pl.ds(pl.multiple_of(tx[q] * ff_t, ff_t), ff_t)

    sends = []

    def remote(src, dst, ss, rs, r, q):
        c = pltpu.make_async_remote_copy(
            src_ref=src, dst_ref=dst, send_sem=ss, recv_sem=rs,
            device_id=(g, ex[r], tx[q]), device_id_type=MESH,
        )
        c.start()
        sends.append(c)
        return c

    def move(src, dst, sem):
        c = pltpu.make_async_copy(src, dst, sem)
        c.start()
        return c

    barrier = pltpu.get_barrier_semaphore()
    for r in range(n_exp):
        for q in range(n_ten):
            if r or q:
                pl.semaphore_signal(
                    barrier, inc=1, device_id=(g, ex[r], tx[q]), device_id_type=MESH
                )

    loads = [
        move(hbm, vmem, l_s.at[5 + j])
        for j, (hbm, vmem) in enumerate(((h_tok, tok), (h_cot, cot), (h_wg, wg), (h_wu, wu)))
    ]
    locs = {"w": move(h_wd.at[0, :, dcol(0)], wdf.at[dff(0), :], l_s.at[2])}

    id0, id1 = ids[0:1, :], ids[1:2, :]
    lab = lax.broadcasted_iota(jnp.int32, (8, toks), 0)
    oh0 = (jnp.broadcast_to(id0, (8, toks)) == lab).astype(jnp.float32)
    oh1 = (jnp.broadcast_to(id1, (8, toks)) == lab).astype(jnp.float32)
    before = (
        lax.broadcasted_iota(jnp.int32, (toks, toks), 0)
        < lax.broadcasted_iota(jnp.int32, (toks, toks), 1)
    ).astype(jnp.bfloat16)
    count = dot((oh0 + oh1).astype(jnp.bfloat16), before)
    p0 = jnp.sum(oh0 * count, axis=0, keepdims=True)
    p1 = jnp.sum(oh1 * (count + oh0), axis=0, keepdims=True)
    none = -1.0
    s0 = jnp.where(p0 < cap, id0.astype(jnp.float32) * cap + p0, none)
    s1 = jnp.where(p1 < cap, id1.astype(jnp.float32) * cap + p1, none)
    gate0, gate1 = gat[0:1, :], gat[1:2, :]

    def place(r):
        slot = (ex[r] * cap + lax.broadcasted_iota(jnp.int32, (cap, toks), 0)).astype(jnp.float32)
        return slot == jnp.broadcast_to(s0, (cap, toks)), slot == jnp.broadcast_to(s1, (cap, toks))

    masks = {r: place(r) for r in range(n_exp)}
    picks = {r: (masks[r][0] | masks[r][1]).astype(jnp.bfloat16) for r in range(n_exp)}
    disp, cp, rcp = {}, {}, {}

    def gather_rows(r):
        srow[r] = dot(picks[r], tok[...]).astype(jnp.bfloat16)

    def gather_cot(r):
        m0, m1 = masks[r]
        scale = jnp.sum(
            jnp.where(m0, jnp.broadcast_to(gate0, m0.shape), 0.0)
            + jnp.where(m1, jnp.broadcast_to(gate1, m1.shape), 0.0),
            axis=1, keepdims=True,
        )
        scot[r] = (scale * dot(picks[r], cot[...])).astype(jnp.bfloat16)

    def dispatch(r, qs, ks=(0, 1)):
        for q in qs:
            for k in ks:
                sb, rb = ((srow, rrow), (scot, rcot))[k]
                src = sb.at[r, :, dcol(q)]
                dst = rb.at[r, drow(0), :]
                if r or q:
                    disp[k, r, q] = remote(src, dst, d_ss.at[k, r, q], d_rs.at[k, r, q], r, q)
                else:
                    locs["d", k] = move(src, dst, l_s.at[k])

    def arrive(r):
        for q in range(n_ten):
            for k in range(2):
                if r or q:
                    disp[k, r, q].wait_recv()
                else:
                    locs["d", k].wait()

    odd = t % 2
    mine = pl.ds(pl.multiple_of(odd * half, half), half)
    other = pl.ds(pl.multiple_of((1 - odd) * half, half), half)

    def partial(r):
        x = rrow[r]
        part[r, 0] = dot(x, wg[0])
        part[r, 1] = dot(x, wu[0])
        part[r, 2] = contract_last(rcot[r], wdf[...])
        cp["a", r] = remote(part.at[r, :, other, :], par.at[r], a_ss.at[r], a_rs.at[r], 0, 1)

    def cross(r):
        cp["a", r].wait_recv()
        total = part[r, :, mine, :] + par[r]
        par[r] = total
        pbs[r] = total.astype(jnp.bfloat16)
        cp["b", r] = remote(pbs.at[r], pbr.at[r], b_ss.at[r], b_rs.at[r], 0, 2)

    def activate(r):
        cp["b", r].wait_recv()
        total = par[r] + pbr[r].astype(jnp.float32)
        pre_gate, pre_up, grad_hidden = total[0], total[1], total[2]
        sig = jax.nn.sigmoid(pre_gate)
        silu = pre_gate * sig
        act[r, 0, mine, :] = (silu * pre_up).astype(jnp.bfloat16)
        act[r, 1, mine, :] = (
            grad_hidden * pre_up * sig * (1.0 + pre_gate * (1.0 - sig))
        ).astype(jnp.bfloat16)
        act[r, 2, mine, :] = (grad_hidden * silu).astype(jnp.bfloat16)
        cp["c", r] = remote(
            act.at[r, :, mine, :], act.at[r, :, mine, :], c_ss.at[r], c_rs.at[r], 0, 1
        )

    def rows_back(r):
        cp["c", r].wait_recv()
        rets[r] = (contract_last(act[r, 1], wg[0]) + contract_last(act[r, 2], wu[0])).astype(
            jnp.bfloat16
        )

    def give_back(r, qs):
        for q in qs:
            src = rets.at[r, drow(q), :]
            dst = retr.at[r, :, dcol(0)]
            if r or q:
                rcp[r, q] = remote(src, dst, r_ss.at[r, q], r_rs.at[r, q], r, q)
            else:
                locs["r"] = move(src, dst, l_s.at[3])

    near, far = (1, 0), (3, 2)
    loads[0].wait()
    gather_rows(2)
    pl.semaphore_wait(barrier, n_exp * n_ten - 1)
    dispatch(2, near, (0,))
    wcp = {
        q: remote(h_wd.at[0, :, dcol(q)], wdf.at[dff(0), :], w_ss.at[q], w_rs.at[q], 0, q)
        for q in (3, 2, 1)
    }
    loads[1].wait()
    gather_cot(2)
    dispatch(2, near, (1,))
    gather_rows(0)
    dispatch(0, far + near, (0,))
    gather_cot(0)
    dispatch(0, far + near, (1,))
    dispatch(2, far)
    for r in (3, 1):
        gather_rows(r)
        gather_cot(r)
    arrive(0)
    loads[2].wait()
    loads[3].wait()
    locs["w"].wait()
    for q in range(1, n_ten):
        wcp[q].wait_recv()
    partial(0)

    arrive(2)
    dispatch(3, near)
    partial(2)
    cross(2)
    cross(0)
    dispatch(1, far)
    dispatch(3, far)
    dispatch(1, near)
    activate(2)
    activate(0)
    rows_back(2)
    rows_back(0)
    give_back(0, near)

    arrive(3)
    give_back(2, near)
    partial(3)
    arrive(1)
    partial(1)
    cross(3)
    cross(1)
    give_back(2, far)
    give_back(0, far)
    activate(3)
    activate(1)
    rows_back(3)
    give_back(3, near)
    rows_back(1)
    give_back(1, far + near)

    slots = n_exp * n_ten * cap
    wide = act.shape[3]
    cot_all = rcot[...].reshape(slots, cols)
    hid = act[:, 0].reshape(slots, wide)
    gds[...] = contract_first(hid, cot_all).astype(jnp.bfloat16)
    gcp = {}
    for q in (3, 2, 1, 0):
        src = gds.at[dff(q), :]
        dst = gdr.at[:, dcol(0)]
        if q:
            gcp[q] = remote(src, dst, g_ss.at[q], g_rs.at[q], 0, q)
        else:
            locs["g"] = move(src, dst, l_s.at[4])
    give_back(3, far)
    rows_all = rrow[...].reshape(slots, cols)
    gg[0] = contract_first(rows_all, act[:, 1].reshape(slots, wide)).astype(jnp.bfloat16)
    gu[0] = contract_first(rows_all, act[:, 2].reshape(slots, wide)).astype(jnp.bfloat16)

    locs["g"].wait()
    for q in range(1, n_ten):
        gcp[q].wait_recv()
    gd[0] = gdr[...]
    locs["r"].wait()
    for r in range(n_exp):
        for q in range(n_ten):
            if r or q:
                rcp[r, q].wait_recv()
    pick = jnp.concatenate([picks[r] for r in range(n_exp)], axis=0)
    ig[...] = contract_first(pick, retr[...].reshape(n_exp * cap, width)).astype(jnp.bfloat16)
    for c in sends:
        c.wait_send()


def fused(tokens, cotangent, expert_ids, gate_wts, w_gate, w_up, w_down):
    toks, width = tokens.shape
    n = 4
    cap = 2 * toks // n
    cols = w_gate.shape[1]
    wide = w_gate.shape[2]
    half = n * cap // 2
    bf, f32 = jnp.bfloat16, jnp.float32
    dma = pltpu.SemaphoreType.DMA
    vmem = pl.BlockSpec(memory_space=pltpu.VMEM)
    hbm = pl.BlockSpec(memory_space=pltpu.HBM)
    return pl.pallas_call(
        kernel,
        out_shape=(
            jax.ShapeDtypeStruct(tokens.shape, bf),
            jax.ShapeDtypeStruct(w_gate.shape, bf),
            jax.ShapeDtypeStruct(w_up.shape, bf),
            jax.ShapeDtypeStruct(w_down.shape, bf),
        ),
        in_specs=[hbm, hbm, vmem, vmem, hbm, hbm, hbm],
        out_specs=(vmem,) * 4,
        scratch_shapes=[
            pltpu.VMEM(tokens.shape, bf),
            pltpu.VMEM(tokens.shape, bf),
            pltpu.VMEM(w_gate.shape, bf),
            pltpu.VMEM(w_up.shape, bf),
            pltpu.VMEM((n, cap, width), bf),
            pltpu.VMEM((n, cap, width), bf),
            pltpu.VMEM((n, n * cap, cols), bf),
            pltpu.VMEM((n, n * cap, cols), bf),
            pltpu.VMEM((wide, cols), bf),
            pltpu.VMEM((n, 3, n * cap, wide), f32),
            pltpu.VMEM((n, 3, half, wide), f32),
            pltpu.VMEM((n, 3, half, wide), bf),
            pltpu.VMEM((n, 3, half, wide), bf),
            pltpu.VMEM((n, 3, n * cap, wide), bf),
            pltpu.VMEM((n, n * cap, cols), bf),
            pltpu.VMEM((n, cap, width), bf),
            pltpu.VMEM((wide, cols), bf),
            pltpu.VMEM(w_down.shape[1:], bf),
            dma((2, n, n)), dma((2, n, n)),
            dma((n,)), dma((n,)),
            dma((n,)), dma((n,)),
            dma((n,)), dma((n,)),
            dma((n,)), dma((n,)),
            dma((n, n)), dma((n, n)),
            dma((n,)), dma((n,)),
            dma((9,)),
        ],
        compiler_params=pltpu.CompilerParams(
            collective_id=0, has_side_effects=True, vmem_limit_bytes=67043328
        ),
        name="expert_backward",
    )(tokens, cotangent, expert_ids.T, gate_wts.T, w_gate, w_up, w_down)


def plain(tokens, cotangent, expert_ids, gate_wts, w_gate, w_up, w_down):
    tok_rows, model_width = tokens.shape
    experts = lax.axis_size("expert")
    capacity = 2 * tok_rows // experts
    slots_all = experts * capacity
    zero_half = jnp.zeros((), jnp.bfloat16)
    flat_ids = expert_ids.reshape(-1)
    onehot = (flat_ids[:, None] == jnp.arange(experts, dtype=jnp.int32)[None, :]).astype(jnp.int32)
    positions = jnp.sum(onehot * (jnp.cumsum(onehot, axis=0) - 1), axis=1)
    retained = positions < capacity
    target = jnp.where(retained, flat_ids * capacity + positions, slots_all)
    anchor = (
        jnp.full((slots_all,), -1, jnp.int32)
        .at[target]
        .set(jnp.arange(2 * tok_rows, dtype=jnp.int32), mode="drop")
    )
    populated_rows = anchor >= 0
    picked = jnp.maximum(anchor, 0)
    tok_index = picked // 2
    send_rows = jnp.where(populated_rows[:, None], tokens[tok_index], zero_half)
    gate_scale = gate_wts.reshape(-1)[picked]
    scaled = (gate_scale[:, None] * cotangent[tok_index].astype(jnp.float32)).astype(jnp.bfloat16)
    send_cot = jnp.where(populated_rows[:, None], scaled, zero_half)
    recv_rows, recv_cot = (
        lax.all_to_all(
            send_rows.reshape(experts, capacity, model_width),
            "expert",
            split_axis=0,
            concat_axis=0,
            tiled=True,
        ),
        lax.all_to_all(
            send_cot.reshape(experts, capacity, model_width),
            "expert",
            split_axis=0,
            concat_axis=0,
            tiled=True,
        ),
    )
    rows_in = recv_rows.reshape(slots_all, model_width)
    cot_in = recv_cot.reshape(slots_all, model_width)
    gate_shard = w_gate[0]
    up_shard = w_up[0]
    down_shard = w_down[0]
    hidden_width = gate_shard.shape[1]
    full_gate, full_up, complete_down_weight = (
        lax.all_gather(gate_shard, "tensor", axis=0, tiled=True),
        lax.all_gather(up_shard, "tensor", axis=0, tiled=True),
        lax.all_gather(down_shard, "tensor", axis=0, tiled=True),
    )
    pre_gate = jnp.dot(rows_in, full_gate, preferred_element_type=jnp.float32)
    pre_up = jnp.dot(rows_in, full_up, preferred_element_type=jnp.float32)
    grad_hidden = contract_last(cot_in, complete_down_weight)
    sigmoid_gate = jax.nn.sigmoid(pre_gate)
    activated = pre_gate * sigmoid_gate
    hidden = (activated * pre_up).astype(jnp.bfloat16)
    grad_gate_pre = (
        grad_hidden * pre_up * sigmoid_gate * (1.0 + pre_gate * (1.0 - sigmoid_gate))
    ).astype(jnp.bfloat16)
    grad_up_pre = (grad_hidden * activated).astype(jnp.bfloat16)
    joint_grad = jnp.concatenate([grad_gate_pre, grad_up_pre], axis=1)
    columns = rows_in
    summed = lax.psum_scatter(
        contract_first(columns, joint_grad).astype(jnp.bfloat16),
        "tensor",
        scatter_dimension=0,
        tiled=True,
    ).astype(jnp.float32)
    columns = hidden
    summed_down = lax.psum_scatter(
        contract_first(columns, cot_in).astype(jnp.bfloat16),
        "tensor",
        scatter_dimension=0,
        tiled=True,
    )
    rows_out = (
        contract_last(grad_gate_pre, full_gate) + contract_last(grad_up_pre, full_up)
    ).astype(jnp.bfloat16)
    returned = lax.all_to_all(
        rows_out.reshape(experts, capacity, model_width),
        "expert",
        split_axis=0,
        concat_axis=0,
        tiled=True,
    )
    returned = returned.reshape(slots_all, model_width)
    gathered = returned[jnp.minimum(target, slots_all - 1)].astype(jnp.float32)
    gathered = jnp.where(retained[:, None], gathered, jnp.zeros((), jnp.float32))
    input_grad = jnp.sum(gathered.reshape(tok_rows, 2, model_width), axis=1).astype(jnp.bfloat16)
    return (
        input_grad,
        summed[:, :hidden_width].astype(jnp.bfloat16)[None],
        summed[:, hidden_width:].astype(jnp.bfloat16)[None],
        summed_down[None],
    )


def solution(mesh):
    n_exp, n_ten = mesh.shape["expert"], mesh.shape["tensor"]

    def local(tokens, cotangent, expert_ids, gate_wts, w_gate, w_up, w_down):
        args = (tokens, cotangent, expert_ids, gate_wts, w_gate, w_up, w_down)
        capacity = 2 * tokens.shape[0] // n_exp
        small = n_exp == 4 and n_ten == 4 and capacity % 16 == 0
        return fused(*args) if small else plain(*args)

    return jax.shard_map(
        local,
        mesh=mesh,
        in_specs=(
            P(("group", "expert", "tensor"), None),
            P(("group", "expert", "tensor"), None),
            P(("group", "expert", "tensor"), None),
            P(("group", "expert", "tensor"), None),
            P("expert", "tensor", None),
            P("expert", "tensor", None),
            P("expert", "tensor", None),
        ),
        out_specs=(
            P(("group", "expert", "tensor"), None),
            P(("group", "expert"), "tensor", None),
            P(("group", "expert"), "tensor", None),
            P(("group", "expert"), "tensor", None),
        ),
        check_vma=False,
    )
```

```python
import jax
import jax.numpy as jnp
from jax import lax
from jax.experimental import pallas as pl
from jax.experimental.pallas import tpu as pltpu
from jax.sharding import PartitionSpec as P

MESH = pl.DeviceIdType.MESH


def contract_last(left, right):
    return lax.dot_general(
        left, right, (((1,), (1,)), ((), ())), preferred_element_type=jnp.float32
    )


def contract_first(left, right):
    return lax.dot_general(
        left, right, (((0,), (0,)), ((), ())), preferred_element_type=jnp.float32
    )


def dot(left, right):
    return jnp.dot(left, right, preferred_element_type=jnp.float32)


def flip(index, mask):
    out = index
    for bit in (1, 2):
        if mask & bit:
            out = out + bit - 2 * bit * ((index // bit) % 2)
    return out


def kernel(
    h_tok, h_cot, ids, gat, h_wg, h_wu, h_wd,
    ig, gg, gu, gd,
    tok, cot, wg, wu, srow, scot, rrow, rcot, wdf, part, par, pbs, pbr, act, rets, retr, gds, gdr,
    d_ss, d_rs, w_ss, w_rs, a_ss, a_rs, b_ss, b_rs, c_ss, c_rs, r_ss, r_rs, g_ss, g_rs, l_s,
):
    n_exp, n_ten = 4, 4
    toks, width = tok.shape
    cols = width // n_ten
    cap = srow.shape[1]
    half = n_ten * cap // 2
    ff_t = h_wd.shape[1]
    g = lax.axis_index("group")
    e = lax.axis_index("expert")
    t = lax.axis_index("tensor")
    ex = [flip(e, r) for r in range(n_exp)]
    tx = [flip(t, q) for q in range(n_ten)]

    def dcol(q):
        return pl.ds(pl.multiple_of(tx[q] * cols, cols), cols)

    def drow(q):
        return pl.ds(pl.multiple_of(tx[q] * cap, cap), cap)

    def dff(q):
        return pl.ds(pl.multiple_of(tx[q] * ff_t, ff_t), ff_t)

    sends = []

    def remote(src, dst, ss, rs, r, q):
        c = pltpu.make_async_remote_copy(
            src_ref=src, dst_ref=dst, send_sem=ss, recv_sem=rs,
            device_id=(g, ex[r], tx[q]), device_id_type=MESH,
        )
        c.start()
        sends.append(c)
        return c

    def move(src, dst, sem):
        c = pltpu.make_async_copy(src, dst, sem)
        c.start()
        return c

    barrier = pltpu.get_barrier_semaphore()
    for r in range(n_exp):
        for q in range(n_ten):
            if r or q:
                pl.semaphore_signal(
                    barrier, inc=1, device_id=(g, ex[r], tx[q]), device_id_type=MESH
                )

    loads = [
        move(hbm, vmem, l_s.at[5 + j])
        for j, (hbm, vmem) in enumerate(((h_tok, tok), (h_cot, cot), (h_wg, wg), (h_wu, wu)))
    ]
    locs = {"w": move(h_wd.at[0, :, dcol(0)], wdf.at[dff(0), :], l_s.at[2])}

    id0, id1 = ids[0:1, :], ids[1:2, :]
    lab = lax.broadcasted_iota(jnp.int32, (8, toks), 0)
    oh0 = (jnp.broadcast_to(id0, (8, toks)) == lab).astype(jnp.float32)
    oh1 = (jnp.broadcast_to(id1, (8, toks)) == lab).astype(jnp.float32)
    before = (
        lax.broadcasted_iota(jnp.int32, (toks, toks), 0)
        < lax.broadcasted_iota(jnp.int32, (toks, toks), 1)
    ).astype(jnp.bfloat16)
    count = dot((oh0 + oh1).astype(jnp.bfloat16), before)
    p0 = jnp.sum(oh0 * count, axis=0, keepdims=True)
    p1 = jnp.sum(oh1 * (count + oh0), axis=0, keepdims=True)
    none = -1.0
    s0 = jnp.where(p0 < cap, id0.astype(jnp.float32) * cap + p0, none)
    s1 = jnp.where(p1 < cap, id1.astype(jnp.float32) * cap + p1, none)
    gate0, gate1 = gat[0:1, :], gat[1:2, :]

    def place(r):
        slot = (ex[r] * cap + lax.broadcasted_iota(jnp.int32, (cap, toks), 0)).astype(jnp.float32)
        return slot == jnp.broadcast_to(s0, (cap, toks)), slot == jnp.broadcast_to(s1, (cap, toks))

    masks = {r: place(r) for r in range(n_exp)}
    picks = {r: (masks[r][0] | masks[r][1]).astype(jnp.bfloat16) for r in range(n_exp)}
    disp, cp, rcp = {}, {}, {}

    def gather_rows(r):
        srow[r] = dot(picks[r], tok[...]).astype(jnp.bfloat16)

    def gather_cot(r):
        m0, m1 = masks[r]
        scale = jnp.sum(
            jnp.where(m0, jnp.broadcast_to(gate0, m0.shape), 0.0)
            + jnp.where(m1, jnp.broadcast_to(gate1, m1.shape), 0.0),
            axis=1, keepdims=True,
        )
        scot[r] = (scale * dot(picks[r], cot[...])).astype(jnp.bfloat16)

    def dispatch(r, qs, ks=(0, 1)):
        for q in qs:
            for k in ks:
                sb, rb = ((srow, rrow), (scot, rcot))[k]
                src = sb.at[r, :, dcol(q)]
                dst = rb.at[r, drow(0), :]
                if r or q:
                    disp[k, r, q] = remote(src, dst, d_ss.at[k, r, q], d_rs.at[k, r, q], r, q)
                else:
                    locs["d", k] = move(src, dst, l_s.at[k])

    def arrive(r):
        for q in range(n_ten):
            for k in range(2):
                if r or q:
                    disp[k, r, q].wait_recv()
                else:
                    locs["d", k].wait()

    odd = t % 2
    mine = pl.ds(pl.multiple_of(odd * half, half), half)
    other = pl.ds(pl.multiple_of((1 - odd) * half, half), half)

    def partial(r):
        x = rrow[r]
        part[r, 0] = dot(x, wg[0])
        part[r, 1] = dot(x, wu[0])
        part[r, 2] = contract_last(rcot[r], wdf[...])
        cp["a", r] = remote(part.at[r, :, other, :], par.at[r], a_ss.at[r], a_rs.at[r], 0, 1)

    def cross(r):
        cp["a", r].wait_recv()
        total = part[r, :, mine, :] + par[r]
        par[r] = total
        pbs[r] = total.astype(jnp.bfloat16)
        cp["b", r] = remote(pbs.at[r], pbr.at[r], b_ss.at[r], b_rs.at[r], 0, 2)

    def activate(r):
        cp["b", r].wait_recv()
        total = par[r] + pbr[r].astype(jnp.float32)
        pre_gate, pre_up, grad_hidden = total[0], total[1], total[2]
        sig = jax.nn.sigmoid(pre_gate)
        silu = pre_gate * sig
        act[r, 0, mine, :] = (silu * pre_up).astype(jnp.bfloat16)
        act[r, 1, mine, :] = (
            grad_hidden * pre_up * sig * (1.0 + pre_gate * (1.0 - sig))
        ).astype(jnp.bfloat16)
        act[r, 2, mine, :] = (grad_hidden * silu).astype(jnp.bfloat16)
        cp["c", r] = remote(
            act.at[r, :, mine, :], act.at[r, :, mine, :], c_ss.at[r], c_rs.at[r], 0, 1
        )

    def rows_back(r):
        cp["c", r].wait_recv()
        rets[r] = (contract_last(act[r, 1], wg[0]) + contract_last(act[r, 2], wu[0])).astype(
            jnp.bfloat16
        )

    def give_back(r, qs):
        for q in qs:
            src = rets.at[r, drow(q), :]
            dst = retr.at[r, :, dcol(0)]
            if r or q:
                rcp[r, q] = remote(src, dst, r_ss.at[r, q], r_rs.at[r, q], r, q)
            else:
                locs["r"] = move(src, dst, l_s.at[3])

    near, far = (1, 0), (3, 2)
    loads[0].wait()
    gather_rows(2)
    pl.semaphore_wait(barrier, n_exp * n_ten - 1)
    dispatch(2, near, (0,))
    wcp = {
        q: remote(h_wd.at[0, :, dcol(q)], wdf.at[dff(0), :], w_ss.at[q], w_rs.at[q], 0, q)
        for q in (3, 2, 1)
    }
    loads[1].wait()
    gather_cot(2)
    dispatch(2, near, (1,))
    gather_rows(0)
    dispatch(0, far + near, (0,))
    gather_cot(0)
    dispatch(0, far + near, (1,))
    dispatch(2, far)
    gather_rows(1)
    gather_cot(1)
    dispatch(1, far)
    gather_rows(3)
    gather_cot(3)
    arrive(0)
    loads[2].wait()
    loads[3].wait()
    locs["w"].wait()
    for q in range(1, n_ten):
        wcp[q].wait_recv()
    partial(0)

    arrive(2)
    dispatch(3, near)
    partial(2)
    dispatch(1, near)
    cross(2)
    cross(0)
    dispatch(3, far)
    activate(2)
    activate(0)
    rows_back(2)
    rows_back(0)
    give_back(0, far + near)
    arrive(1)
    partial(1)
    cross(1)

    arrive(3)
    give_back(2, near)
    partial(3)
    cross(3)
    give_back(2, far)
    activate(1)
    activate(3)
    rows_back(1)
    give_back(1, far + near)
    rows_back(3)
    give_back(3, near + far)

    slots = n_exp * n_ten * cap
    wide = act.shape[3]
    cot_all = rcot[...].reshape(slots, cols)
    hid = act[:, 0].reshape(slots, wide)
    gds[...] = contract_first(hid, cot_all).astype(jnp.bfloat16)
    gcp = {}
    for q in (3, 2, 1, 0):
        src = gds.at[dff(q), :]
        dst = gdr.at[:, dcol(0)]
        if q:
            gcp[q] = remote(src, dst, g_ss.at[q], g_rs.at[q], 0, q)
        else:
            locs["g"] = move(src, dst, l_s.at[4])
    rows_all = rrow[...].reshape(slots, cols)
    gg[0] = contract_first(rows_all, act[:, 1].reshape(slots, wide)).astype(jnp.bfloat16)
    gu[0] = contract_first(rows_all, act[:, 2].reshape(slots, wide)).astype(jnp.bfloat16)

    locs["g"].wait()
    for q in range(1, n_ten):
        gcp[q].wait_recv()
    gd[0] = gdr[...]
    locs["r"].wait()
    for r in range(n_exp):
        for q in range(n_ten):
            if r or q:
                rcp[r, q].wait_recv()
    pick = jnp.concatenate([picks[r] for r in range(n_exp)], axis=0)
    ig[...] = contract_first(pick, retr[...].reshape(n_exp * cap, width)).astype(jnp.bfloat16)
    for c in sends:
        c.wait_send()


def store(*refs):
    sems = refs[8]
    copies = [pltpu.make_async_copy(refs[j], refs[4 + j], sems.at[j]) for j in range(4)]
    for c in copies:
        c.start()
    for c in copies:
        c.wait()


def fused(tokens, cotangent, expert_ids, gate_wts, w_gate, w_up, w_down):
    toks, width = tokens.shape
    n = 4
    cap = 2 * toks // n
    cols = w_gate.shape[1]
    wide = w_gate.shape[2]
    half = n * cap // 2
    bf, f32 = jnp.bfloat16, jnp.float32
    dma = pltpu.SemaphoreType.DMA
    vmem = pl.BlockSpec(memory_space=pltpu.VMEM)
    hbm = pl.BlockSpec(memory_space=pltpu.HBM)
    results = pl.pallas_call(
        kernel,
        out_shape=(
            pltpu.VMEM(tokens.shape, bf),
            pltpu.VMEM(w_gate.shape, bf),
            pltpu.VMEM(w_up.shape, bf),
            pltpu.VMEM(w_down.shape, bf),
        ),
        in_specs=[hbm, hbm, vmem, vmem, hbm, hbm, hbm],
        out_specs=(vmem,) * 4,
        scratch_shapes=[
            pltpu.VMEM(tokens.shape, bf),
            pltpu.VMEM(tokens.shape, bf),
            pltpu.VMEM(w_gate.shape, bf),
            pltpu.VMEM(w_up.shape, bf),
            pltpu.VMEM((n, cap, width), bf),
            pltpu.VMEM((n, cap, width), bf),
            pltpu.VMEM((n, n * cap, cols), bf),
            pltpu.VMEM((n, n * cap, cols), bf),
            pltpu.VMEM((wide, cols), bf),
            pltpu.VMEM((n, 3, n * cap, wide), f32),
            pltpu.VMEM((n, 3, half, wide), f32),
            pltpu.VMEM((n, 3, half, wide), bf),
            pltpu.VMEM((n, 3, half, wide), bf),
            pltpu.VMEM((n, 3, n * cap, wide), bf),
            pltpu.VMEM((n, n * cap, cols), bf),
            pltpu.VMEM((n, cap, width), bf),
            pltpu.VMEM((wide, cols), bf),
            pltpu.VMEM(w_down.shape[1:], bf),
            dma((2, n, n)), dma((2, n, n)),
            dma((n,)), dma((n,)),
            dma((n,)), dma((n,)),
            dma((n,)), dma((n,)),
            dma((n,)), dma((n,)),
            dma((n, n)), dma((n, n)),
            dma((n,)), dma((n,)),
            dma((9,)),
        ],
        compiler_params=pltpu.CompilerParams(
            collective_id=0, has_side_effects=True, vmem_limit_bytes=62849024
        ),
        name="expert_backward",
    )(tokens, cotangent, expert_ids.T, gate_wts.T, w_gate, w_up, w_down)
    return pl.pallas_call(
        store,
        out_shape=tuple(jax.ShapeDtypeStruct(a.shape, a.dtype) for a in results),
        in_specs=[pl.BlockSpec(memory_space=pl.ANY)] * 4,
        out_specs=(hbm,) * 4,
        scratch_shapes=[dma((4,))],
        compiler_params=pltpu.CompilerParams(vmem_limit_bytes=4 * 1024 * 1024),
        name="store_results",
    )(*results)


def plain(tokens, cotangent, expert_ids, gate_wts, w_gate, w_up, w_down):
    tok_rows, model_width = tokens.shape
    experts = lax.axis_size("expert")
    capacity = 2 * tok_rows // experts
    slots_all = experts * capacity
    zero_half = jnp.zeros((), jnp.bfloat16)
    flat_ids = expert_ids.reshape(-1)
    onehot = (flat_ids[:, None] == jnp.arange(experts, dtype=jnp.int32)[None, :]).astype(jnp.int32)
    positions = jnp.sum(onehot * (jnp.cumsum(onehot, axis=0) - 1), axis=1)
    retained = positions < capacity
    target = jnp.where(retained, flat_ids * capacity + positions, slots_all)
    anchor = (
        jnp.full((slots_all,), -1, jnp.int32)
        .at[target]
        .set(jnp.arange(2 * tok_rows, dtype=jnp.int32), mode="drop")
    )
    populated_rows = anchor >= 0
    picked = jnp.maximum(anchor, 0)
    tok_index = picked // 2
    send_rows = jnp.where(populated_rows[:, None], tokens[tok_index], zero_half)
    gate_scale = gate_wts.reshape(-1)[picked]
    scaled = (gate_scale[:, None] * cotangent[tok_index].astype(jnp.float32)).astype(jnp.bfloat16)
    send_cot = jnp.where(populated_rows[:, None], scaled, zero_half)
    recv_rows, recv_cot = (
        lax.all_to_all(
            send_rows.reshape(experts, capacity, model_width),
            "expert",
            split_axis=0,
            concat_axis=0,
            tiled=True,
        ),
        lax.all_to_all(
            send_cot.reshape(experts, capacity, model_width),
            "expert",
            split_axis=0,
            concat_axis=0,
            tiled=True,
        ),
    )
    rows_in = recv_rows.reshape(slots_all, model_width)
    cot_in = recv_cot.reshape(slots_all, model_width)
    gate_shard = w_gate[0]
    up_shard = w_up[0]
    down_shard = w_down[0]
    hidden_width = gate_shard.shape[1]
    full_gate, full_up, complete_down_weight = (
        lax.all_gather(gate_shard, "tensor", axis=0, tiled=True),
        lax.all_gather(up_shard, "tensor", axis=0, tiled=True),
        lax.all_gather(down_shard, "tensor", axis=0, tiled=True),
    )
    pre_gate = jnp.dot(rows_in, full_gate, preferred_element_type=jnp.float32)
    pre_up = jnp.dot(rows_in, full_up, preferred_element_type=jnp.float32)
    grad_hidden = contract_last(cot_in, complete_down_weight)
    sigmoid_gate = jax.nn.sigmoid(pre_gate)
    activated = pre_gate * sigmoid_gate
    hidden = (activated * pre_up).astype(jnp.bfloat16)
    grad_gate_pre = (
        grad_hidden * pre_up * sigmoid_gate * (1.0 + pre_gate * (1.0 - sigmoid_gate))
    ).astype(jnp.bfloat16)
    grad_up_pre = (grad_hidden * activated).astype(jnp.bfloat16)
    joint_grad = jnp.concatenate([grad_gate_pre, grad_up_pre], axis=1)
    columns = rows_in
    summed = lax.psum_scatter(
        contract_first(columns, joint_grad).astype(jnp.bfloat16),
        "tensor",
        scatter_dimension=0,
        tiled=True,
    ).astype(jnp.float32)
    columns = hidden
    summed_down = lax.psum_scatter(
        contract_first(columns, cot_in).astype(jnp.bfloat16),
        "tensor",
        scatter_dimension=0,
        tiled=True,
    )
    rows_out = (
        contract_last(grad_gate_pre, full_gate) + contract_last(grad_up_pre, full_up)
    ).astype(jnp.bfloat16)
    returned = lax.all_to_all(
        rows_out.reshape(experts, capacity, model_width),
        "expert",
        split_axis=0,
        concat_axis=0,
        tiled=True,
    )
    returned = returned.reshape(slots_all, model_width)
    gathered = returned[jnp.minimum(target, slots_all - 1)].astype(jnp.float32)
    gathered = jnp.where(retained[:, None], gathered, jnp.zeros((), jnp.float32))
    input_grad = jnp.sum(gathered.reshape(tok_rows, 2, model_width), axis=1).astype(jnp.bfloat16)
    return (
        input_grad,
        summed[:, :hidden_width].astype(jnp.bfloat16)[None],
        summed[:, hidden_width:].astype(jnp.bfloat16)[None],
        summed_down[None],
    )


def solution(mesh):
    n_exp, n_ten = mesh.shape["expert"], mesh.shape["tensor"]

    def local(tokens, cotangent, expert_ids, gate_wts, w_gate, w_up, w_down):
        args = (tokens, cotangent, expert_ids, gate_wts, w_gate, w_up, w_down)
        capacity = 2 * tokens.shape[0] // n_exp
        small = n_exp == 4 and n_ten == 4 and capacity % 16 == 0
        return fused(*args) if small else plain(*args)

    return jax.shard_map(
        local,
        mesh=mesh,
        in_specs=(
            P(("group", "expert", "tensor"), None),
            P(("group", "expert", "tensor"), None),
            P(("group", "expert", "tensor"), None),
            P(("group", "expert", "tensor"), None),
            P("expert", "tensor", None),
            P("expert", "tensor", None),
            P("expert", "tensor", None),
        ),
        out_specs=(
            P(("group", "expert", "tensor"), None),
            P(("group", "expert"), "tensor", None),
            P(("group", "expert"), "tensor", None),
            P(("group", "expert"), "tensor", None),
        ),
        check_vma=False,
    )
```

```python
import jax
import jax.numpy as jnp
from jax import lax
from jax.experimental import pallas as pl
from jax.experimental.pallas import tpu as pltpu
from jax.sharding import PartitionSpec as P

MESH = pl.DeviceIdType.MESH


def contract_last(left, right):
    return lax.dot_general(
        left, right, (((1,), (1,)), ((), ())), preferred_element_type=jnp.float32
    )


def contract_first(left, right):
    return lax.dot_general(
        left, right, (((0,), (0,)), ((), ())), preferred_element_type=jnp.float32
    )


def dot(left, right):
    return jnp.dot(left, right, preferred_element_type=jnp.float32)


def flip(index, mask):
    out = index
    for bit in (1, 2):
        if mask & bit:
            out = out + bit - 2 * bit * ((index // bit) % 2)
    return out


def kernel(
    h_tok, h_cot, ids, gat, h_wg, h_wu, h_wd,
    ig, gg, gu, gd,
    tok, cot, wg, wu, srow, scot, rrow, rcot, wdf, part, par, pbs, pbr, act, rets, retr, gds, gdr,
    d_ss, d_rs, w_ss, w_rs, a_ss, a_rs, b_ss, b_rs, c_ss, c_rs, r_ss, r_rs, g_ss, g_rs, l_s,
):
    n_exp, n_ten = 4, 4
    toks, width = tok.shape
    cols = width // n_ten
    cap = srow.shape[1]
    half = n_ten * cap // 2
    ff_t = h_wd.shape[1]
    g = lax.axis_index("group")
    e = lax.axis_index("expert")
    t = lax.axis_index("tensor")
    ex = [flip(e, r) for r in range(n_exp)]
    tx = [flip(t, q) for q in range(n_ten)]

    def dcol(q):
        return pl.ds(pl.multiple_of(tx[q] * cols, cols), cols)

    def drow(q):
        return pl.ds(pl.multiple_of(tx[q] * cap, cap), cap)

    def dff(q):
        return pl.ds(pl.multiple_of(tx[q] * ff_t, ff_t), ff_t)

    sends = []

    def remote(src, dst, ss, rs, r, q):
        c = pltpu.make_async_remote_copy(
            src_ref=src, dst_ref=dst, send_sem=ss, recv_sem=rs,
            device_id=(g, ex[r], tx[q]), device_id_type=MESH,
        )
        c.start()
        sends.append(c)
        return c

    def move(src, dst, sem):
        c = pltpu.make_async_copy(src, dst, sem)
        c.start()
        return c

    barrier = pltpu.get_barrier_semaphore()
    for r in range(n_exp):
        for q in range(n_ten):
            if r or q:
                pl.semaphore_signal(
                    barrier, inc=1, device_id=(g, ex[r], tx[q]), device_id_type=MESH
                )

    loads = [
        move(hbm, vmem, l_s.at[5 + j])
        for j, (hbm, vmem) in enumerate(((h_tok, tok), (h_cot, cot), (h_wg, wg), (h_wu, wu)))
    ]
    locs = {"w": move(h_wd.at[0, :, dcol(0)], wdf.at[dff(0), :], l_s.at[2])}

    id0, id1 = ids[0:1, :], ids[1:2, :]
    lab = lax.broadcasted_iota(jnp.int32, (8, toks), 0)
    oh0 = (jnp.broadcast_to(id0, (8, toks)) == lab).astype(jnp.float32)
    oh1 = (jnp.broadcast_to(id1, (8, toks)) == lab).astype(jnp.float32)
    before = (
        lax.broadcasted_iota(jnp.int32, (toks, toks), 0)
        < lax.broadcasted_iota(jnp.int32, (toks, toks), 1)
    ).astype(jnp.bfloat16)
    count = dot((oh0 + oh1).astype(jnp.bfloat16), before)
    p0 = jnp.sum(oh0 * count, axis=0, keepdims=True)
    p1 = jnp.sum(oh1 * (count + oh0), axis=0, keepdims=True)
    none = -1.0
    s0 = jnp.where(p0 < cap, id0.astype(jnp.float32) * cap + p0, none)
    s1 = jnp.where(p1 < cap, id1.astype(jnp.float32) * cap + p1, none)
    gate0, gate1 = gat[0:1, :], gat[1:2, :]

    def place(r):
        slot = (ex[r] * cap + lax.broadcasted_iota(jnp.int32, (cap, toks), 0)).astype(jnp.float32)
        return slot == jnp.broadcast_to(s0, (cap, toks)), slot == jnp.broadcast_to(s1, (cap, toks))

    masks = {r: place(r) for r in range(n_exp)}
    picks = {r: (masks[r][0] | masks[r][1]).astype(jnp.bfloat16) for r in range(n_exp)}
    disp, cp, rcp = {}, {}, {}

    def gather_rows(r):
        srow[r] = dot(picks[r], tok[...]).astype(jnp.bfloat16)

    def gather_cot(r):
        m0, m1 = masks[r]
        scale = jnp.sum(
            jnp.where(m0, jnp.broadcast_to(gate0, m0.shape), 0.0)
            + jnp.where(m1, jnp.broadcast_to(gate1, m1.shape), 0.0),
            axis=1, keepdims=True,
        )
        scot[r] = (scale * dot(picks[r], cot[...])).astype(jnp.bfloat16)

    def dispatch(r, qs, ks=(0, 1)):
        for q in qs:
            for k in ks:
                sb, rb = ((srow, rrow), (scot, rcot))[k]
                src = sb.at[r, :, dcol(q)]
                dst = rb.at[r, drow(0), :]
                if r or q:
                    disp[k, r, q] = remote(src, dst, d_ss.at[k, r, q], d_rs.at[k, r, q], r, q)
                else:
                    locs["d", k] = move(src, dst, l_s.at[k])

    def arrive(r):
        for q in range(n_ten):
            for k in range(2):
                if r or q:
                    disp[k, r, q].wait_recv()
                else:
                    locs["d", k].wait()

    odd = t % 2
    mine = pl.ds(pl.multiple_of(odd * half, half), half)
    other = pl.ds(pl.multiple_of((1 - odd) * half, half), half)

    def partial(r):
        x = rrow[r]
        part[r, 0] = dot(x, wg[0])
        part[r, 1] = dot(x, wu[0])
        part[r, 2] = contract_last(rcot[r], wdf[...])
        cp["a", r] = remote(part.at[r, :, other, :], par.at[r], a_ss.at[r], a_rs.at[r], 0, 1)

    def cross(r):
        cp["a", r].wait_recv()
        total = part[r, :, mine, :] + par[r]
        par[r] = total
        pbs[r] = total.astype(jnp.bfloat16)
        cp["b", r] = remote(pbs.at[r], pbr.at[r], b_ss.at[r], b_rs.at[r], 0, 2)

    def activate(r):
        cp["b", r].wait_recv()
        total = par[r] + pbr[r].astype(jnp.float32)
        pre_gate, pre_up, grad_hidden = total[0], total[1], total[2]
        sig = jax.nn.sigmoid(pre_gate)
        silu = pre_gate * sig
        act[r, 0, mine, :] = (silu * pre_up).astype(jnp.bfloat16)
        act[r, 1, mine, :] = (
            grad_hidden * pre_up * sig * (1.0 + pre_gate * (1.0 - sig))
        ).astype(jnp.bfloat16)
        act[r, 2, mine, :] = (grad_hidden * silu).astype(jnp.bfloat16)
        cp["c", r] = remote(
            act.at[r, :, mine, :], act.at[r, :, mine, :], c_ss.at[r], c_rs.at[r], 0, 1
        )

    def rows_back(r):
        cp["c", r].wait_recv()
        rets[r] = (contract_last(act[r, 1], wg[0]) + contract_last(act[r, 2], wu[0])).astype(
            jnp.bfloat16
        )

    def give_back(r, qs):
        for q in qs:
            src = rets.at[r, drow(q), :]
            dst = retr.at[r, :, dcol(0)]
            if r or q:
                rcp[r, q] = remote(src, dst, r_ss.at[r, q], r_rs.at[r, q], r, q)
            else:
                locs["r"] = move(src, dst, l_s.at[3])

    near, far = (1, 0), (3, 2)
    loads[0].wait()
    gather_rows(2)
    pl.semaphore_wait(barrier, n_exp * n_ten - 1)
    dispatch(2, near, (0,))
    wcp = {
        q: remote(h_wd.at[0, :, dcol(q)], wdf.at[dff(0), :], w_ss.at[q], w_rs.at[q], 0, q)
        for q in (3, 2, 1)
    }
    loads[1].wait()
    gather_cot(2)
    dispatch(2, near, (1,))
    gather_rows(0)
    dispatch(0, far + near, (0,))
    gather_cot(0)
    dispatch(0, far + near, (1,))
    dispatch(2, far)
    for r in (3, 1):
        gather_rows(r)
        gather_cot(r)
    arrive(0)
    loads[2].wait()
    loads[3].wait()
    locs["w"].wait()
    for q in range(1, n_ten):
        wcp[q].wait_recv()
    partial(0)

    arrive(2)
    dispatch(3, near)
    partial(2)
    cross(2)
    cross(0)
    dispatch(1, far)
    dispatch(3, far)
    dispatch(1, near)
    activate(2)
    activate(0)
    rows_back(2)
    rows_back(0)
    give_back(0, near)

    arrive(3)
    give_back(2, near)
    partial(3)
    arrive(1)
    partial(1)
    cross(3)
    cross(1)
    give_back(2, far)
    give_back(0, far)
    activate(3)
    activate(1)
    rows_back(3)
    give_back(3, near)
    rows_back(1)
    give_back(1, far + near)

    slots = n_exp * n_ten * cap
    wide = act.shape[3]
    cot_all = rcot[...].reshape(slots, cols)
    hid = act[:, 0].reshape(slots, wide)
    gds[...] = contract_first(hid, cot_all).astype(jnp.bfloat16)
    gcp = {}
    for q in (3, 2, 1, 0):
        src = gds.at[dff(q), :]
        dst = gdr.at[:, dcol(0)]
        if q:
            gcp[q] = remote(src, dst, g_ss.at[q], g_rs.at[q], 0, q)
        else:
            locs["g"] = move(src, dst, l_s.at[4])
    give_back(3, far)
    rows_all = rrow[...].reshape(slots, cols)
    gg[0] = contract_first(rows_all, act[:, 1].reshape(slots, wide)).astype(jnp.bfloat16)
    gu[0] = contract_first(rows_all, act[:, 2].reshape(slots, wide)).astype(jnp.bfloat16)

    locs["g"].wait()
    for q in range(1, n_ten):
        gcp[q].wait_recv()
    gd[0] = gdr[...]
    locs["r"].wait()
    for r in range(n_exp):
        for q in range(n_ten):
            if r or q:
                rcp[r, q].wait_recv()
    pick = jnp.concatenate([picks[r] for r in range(n_exp)], axis=0)
    ig[...] = contract_first(pick, retr[...].reshape(n_exp * cap, width)).astype(jnp.bfloat16)
    for c in sends:
        c.wait_send()


def store(*refs):
    sems = refs[8]
    copies = [pltpu.make_async_copy(refs[j], refs[4 + j], sems.at[j]) for j in range(4)]
    for c in copies:
        c.start()
    for c in copies:
        c.wait()


def fused(tokens, cotangent, expert_ids, gate_wts, w_gate, w_up, w_down):
    toks, width = tokens.shape
    n = 4
    cap = 2 * toks // n
    cols = w_gate.shape[1]
    wide = w_gate.shape[2]
    half = n * cap // 2
    bf, f32 = jnp.bfloat16, jnp.float32
    dma = pltpu.SemaphoreType.DMA
    vmem = pl.BlockSpec(memory_space=pltpu.VMEM)
    hbm = pl.BlockSpec(memory_space=pltpu.HBM)
    results = pl.pallas_call(
        kernel,
        out_shape=(
            pltpu.VMEM(tokens.shape, bf),
            pltpu.VMEM(w_gate.shape, bf),
            pltpu.VMEM(w_up.shape, bf),
            pltpu.VMEM(w_down.shape, bf),
        ),
        in_specs=[hbm, hbm, vmem, vmem, hbm, hbm, hbm],
        out_specs=(vmem,) * 4,
        scratch_shapes=[
            pltpu.VMEM(tokens.shape, bf),
            pltpu.VMEM(tokens.shape, bf),
            pltpu.VMEM(w_gate.shape, bf),
            pltpu.VMEM(w_up.shape, bf),
            pltpu.VMEM((n, cap, width), bf),
            pltpu.VMEM((n, cap, width), bf),
            pltpu.VMEM((n, n * cap, cols), bf),
            pltpu.VMEM((n, n * cap, cols), bf),
            pltpu.VMEM((wide, cols), bf),
            pltpu.VMEM((n, 3, n * cap, wide), f32),
            pltpu.VMEM((n, 3, half, wide), f32),
            pltpu.VMEM((n, 3, half, wide), bf),
            pltpu.VMEM((n, 3, half, wide), bf),
            pltpu.VMEM((n, 3, n * cap, wide), bf),
            pltpu.VMEM((n, n * cap, cols), bf),
            pltpu.VMEM((n, cap, width), bf),
            pltpu.VMEM((wide, cols), bf),
            pltpu.VMEM(w_down.shape[1:], bf),
            dma((2, n, n)), dma((2, n, n)),
            dma((n,)), dma((n,)),
            dma((n,)), dma((n,)),
            dma((n,)), dma((n,)),
            dma((n,)), dma((n,)),
            dma((n, n)), dma((n, n)),
            dma((n,)), dma((n,)),
            dma((9,)),
        ],
        compiler_params=pltpu.CompilerParams(
            collective_id=0, has_side_effects=True, vmem_limit_bytes=62849024
        ),
        name="expert_backward",
    )(tokens, cotangent, expert_ids.T, gate_wts.T, w_gate, w_up, w_down)
    return pl.pallas_call(
        store,
        out_shape=tuple(jax.ShapeDtypeStruct(a.shape, a.dtype) for a in results),
        in_specs=[pl.BlockSpec(memory_space=pl.ANY)] * 4,
        out_specs=(hbm,) * 4,
        scratch_shapes=[dma((4,))],
        compiler_params=pltpu.CompilerParams(vmem_limit_bytes=4 * 1024 * 1024),
        name="store_results",
    )(*results)


def plain(tokens, cotangent, expert_ids, gate_wts, w_gate, w_up, w_down):
    tok_rows, model_width = tokens.shape
    experts = lax.axis_size("expert")
    capacity = 2 * tok_rows // experts
    slots_all = experts * capacity
    zero_half = jnp.zeros((), jnp.bfloat16)
    flat_ids = expert_ids.reshape(-1)
    onehot = (flat_ids[:, None] == jnp.arange(experts, dtype=jnp.int32)[None, :]).astype(jnp.int32)
    positions = jnp.sum(onehot * (jnp.cumsum(onehot, axis=0) - 1), axis=1)
    retained = positions < capacity
    target = jnp.where(retained, flat_ids * capacity + positions, slots_all)
    anchor = (
        jnp.full((slots_all,), -1, jnp.int32)
        .at[target]
        .set(jnp.arange(2 * tok_rows, dtype=jnp.int32), mode="drop")
    )
    populated_rows = anchor >= 0
    picked = jnp.maximum(anchor, 0)
    tok_index = picked // 2
    send_rows = jnp.where(populated_rows[:, None], tokens[tok_index], zero_half)
    gate_scale = gate_wts.reshape(-1)[picked]
    scaled = (gate_scale[:, None] * cotangent[tok_index].astype(jnp.float32)).astype(jnp.bfloat16)
    send_cot = jnp.where(populated_rows[:, None], scaled, zero_half)
    recv_rows, recv_cot = (
        lax.all_to_all(
            send_rows.reshape(experts, capacity, model_width),
            "expert",
            split_axis=0,
            concat_axis=0,
            tiled=True,
        ),
        lax.all_to_all(
            send_cot.reshape(experts, capacity, model_width),
            "expert",
            split_axis=0,
            concat_axis=0,
            tiled=True,
        ),
    )
    rows_in = recv_rows.reshape(slots_all, model_width)
    cot_in = recv_cot.reshape(slots_all, model_width)
    gate_shard = w_gate[0]
    up_shard = w_up[0]
    down_shard = w_down[0]
    hidden_width = gate_shard.shape[1]
    full_gate, full_up, complete_down_weight = (
        lax.all_gather(gate_shard, "tensor", axis=0, tiled=True),
        lax.all_gather(up_shard, "tensor", axis=0, tiled=True),
        lax.all_gather(down_shard, "tensor", axis=0, tiled=True),
    )
    pre_gate = jnp.dot(rows_in, full_gate, preferred_element_type=jnp.float32)
    pre_up = jnp.dot(rows_in, full_up, preferred_element_type=jnp.float32)
    grad_hidden = contract_last(cot_in, complete_down_weight)
    sigmoid_gate = jax.nn.sigmoid(pre_gate)
    activated = pre_gate * sigmoid_gate
    hidden = (activated * pre_up).astype(jnp.bfloat16)
    grad_gate_pre = (
        grad_hidden * pre_up * sigmoid_gate * (1.0 + pre_gate * (1.0 - sigmoid_gate))
    ).astype(jnp.bfloat16)
    grad_up_pre = (grad_hidden * activated).astype(jnp.bfloat16)
    joint_grad = jnp.concatenate([grad_gate_pre, grad_up_pre], axis=1)
    columns = rows_in
    summed = lax.psum_scatter(
        contract_first(columns, joint_grad).astype(jnp.bfloat16),
        "tensor",
        scatter_dimension=0,
        tiled=True,
    ).astype(jnp.float32)
    columns = hidden
    summed_down = lax.psum_scatter(
        contract_first(columns, cot_in).astype(jnp.bfloat16),
        "tensor",
        scatter_dimension=0,
        tiled=True,
    )
    rows_out = (
        contract_last(grad_gate_pre, full_gate) + contract_last(grad_up_pre, full_up)
    ).astype(jnp.bfloat16)
    returned = lax.all_to_all(
        rows_out.reshape(experts, capacity, model_width),
        "expert",
        split_axis=0,
        concat_axis=0,
        tiled=True,
    )
    returned = returned.reshape(slots_all, model_width)
    gathered = returned[jnp.minimum(target, slots_all - 1)].astype(jnp.float32)
    gathered = jnp.where(retained[:, None], gathered, jnp.zeros((), jnp.float32))
    input_grad = jnp.sum(gathered.reshape(tok_rows, 2, model_width), axis=1).astype(jnp.bfloat16)
    return (
        input_grad,
        summed[:, :hidden_width].astype(jnp.bfloat16)[None],
        summed[:, hidden_width:].astype(jnp.bfloat16)[None],
        summed_down[None],
    )


def solution(mesh):
    n_exp, n_ten = mesh.shape["expert"], mesh.shape["tensor"]

    def local(tokens, cotangent, expert_ids, gate_wts, w_gate, w_up, w_down):
        args = (tokens, cotangent, expert_ids, gate_wts, w_gate, w_up, w_down)
        capacity = 2 * tokens.shape[0] // n_exp
        small = n_exp == 4 and n_ten == 4 and capacity % 16 == 0
        return fused(*args) if small else plain(*args)

    return jax.shard_map(
        local,
        mesh=mesh,
        in_specs=(
            P(("group", "expert", "tensor"), None),
            P(("group", "expert", "tensor"), None),
            P(("group", "expert", "tensor"), None),
            P(("group", "expert", "tensor"), None),
            P("expert", "tensor", None),
            P("expert", "tensor", None),
            P("expert", "tensor", None),
        ),
        out_specs=(
            P(("group", "expert", "tensor"), None),
            P(("group", "expert"), "tensor", None),
            P(("group", "expert"), "tensor", None),
            P(("group", "expert"), "tensor", None),
        ),
        check_vma=False,
    )
```
